32 devices in a mesh: row: 4 (over y, core), col: 8 (over z, x).
Axes of the slice: x: 2, y: 2, z: 4, core: 2. Of those that a mesh axis runs over, the one named last changes fastest.
Arguments:
- blocks: float32 [4096, 128, 128], P(('row', 'col')), may hold values from -0.25 to 0.25
- block_rows: int32 [32, 128], P(('row', 'col')), may hold values from 0 to 1023, as said below
- block_cols: int32 [32, 128], P(('row', 'col')), may hold values from 0 to 511
- diagonal: float32 [524288], P(('row', 'col')), may hold values from 1 to 4
- right_sides: float32 [2, 524288], P(None, ('row', 'col')), may hold values from -6 to 6
Outputs:
- solution: float32 [2, 524288], P(None, ('row', 'col'))
- hessenberg: float32 [2, 9, 8], replicated
The draws below stay inside these ranges and needn't reach their ends.
Inputs may be any that keep to these rules, and one draw needn't show every extreme that they name: `block_rows`: non-decreasing along each tile's slots; a local block row may hold no stored block.
All inputs are finite; a program needn't handle non-finite values.
Results may differ from the reference program's by a relative error of at most 0.0085.
Values sent between devices are 32-bit elements; how exact they have to be, the bound alone decides.
A program may use at most 128 MiB of HBM per device.

```python
import math
import jax
import jax.numpy as jnp
from jax import lax

BS = 128
PB = 128
NRHS = 2
STEPS = 8
TILES = 32
ROWB = 1024
COLB = 512
CAP = 128
NUNK = 524288
N_ROW = 4
N_COL = 8


def draw_block_rows(key, part):
    levels_top = ROWB.bit_length() - 1
    level_key = jax.random.fold_in(key, 11)
    value_key = jax.random.fold_in(key, 12)
    order_key = jax.random.fold_in(key, 13)
    levels = jax.random.randint(level_key, (TILES, CAP), 0, levels_top + 1, dtype=jnp.int32)
    spans = jnp.left_shift(jnp.ones_like(levels), levels)
    raw = jax.random.randint(value_key, (TILES, CAP), 0, spans, dtype=jnp.int32)
    order = jax.random.permutation(order_key, ROWB).astype(jnp.int32)
    placed = jnp.take(order, raw)
    return jnp.sort(placed, axis=1).astype(jnp.int32)


def place_ends(entries, key, low, high):
    index_at = [jax.random.randint(jax.random.fold_in(key, axis), (), 0, length) for axis, length in enumerate(entries.shape)]
    longest = entries.shape.index(max(entries.shape))
    beside = index_at[:longest] + [(index_at[longest] + 1) % entries.shape[longest]] + index_at[longest + 1:]
    return entries.at[tuple(index_at)].set(low).at[tuple(beside)].set(high)


def block_scale(key, dims, split, low, largest):
    loudness = 1.0
    for axis_at, blocks in split:
        heights = jax.random.uniform(jax.random.fold_in(jax.random.fold_in(key, 6), axis_at), (blocks,), jnp.float32, low / len(split), largest / len(split))
        loudness = loudness * jnp.repeat(jnp.exp(heights), dims[axis_at] // blocks).reshape((-1,) + (1,) * (len(dims) - 1 - axis_at))
    return loudness


def bell_draw(key, extent, width, reach, shards=(), held_as=jnp.bfloat16):
    array = width * jax.random.normal(key, extent, jnp.float32)
    if shards:
        array = array * block_scale(key, extent, shards, -0.22, 0.18)
    return jnp.clip(array, -reach, reach).astype(held_as)


def setup_inputs(seed: int = 0) -> dict:
    key_of = jax.random.split(jax.random.key(seed), 6)
    blocks = bell_draw(key_of[0], (TILES * CAP, BS, BS), (4 * BS) ** -0.5, 0.25, ((0, 32),), jnp.float32)
    block_rows = draw_block_rows(jax.random.fold_in(key_of[5], 71), 0)
    block_cols = place_ends(jax.random.randint(key_of[2], (TILES, CAP), 0, COLB), jax.random.fold_in(key_of[2], 1), 0, COLB - 1).astype(jnp.int32)
    diagonal = jnp.clip(jnp.exp(math.log(4.0) - 1.3862944 * jax.random.uniform(key_of[3], (NUNK,), jnp.float32) ** block_scale(key_of[3], (NUNK,), ((0, 32),), -0.2, 0.2)), 1.0, 4.0)
    right_sides = bell_draw(key_of[4], (NRHS, NUNK), 1.0, 6.0, ((1, 32),), jnp.float32)
    return dict(blocks=blocks, block_rows=block_rows, block_cols=block_cols, diagonal=diagonal, right_sides=right_sides)


epsilon = 1e-06

def least_squares(hessenberg, initial_norm):
    total_steps = hessenberg.shape[2]
    targets = [initial_norm] + [jnp.zeros_like(initial_norm) for j in range(total_steps)]
    cosines, sines, triangle = ([], [], [])
    for j in range(total_steps):
        column = [hessenberg[:, i, j] for i in range(j + 2)]
        for i in range(j):
            leading, trailing = (column[i], column[i + 1])
            column[i] = cosines[i] * leading + sines[i] * trailing
            column[i + 1] = cosines[i] * trailing - sines[i] * leading
        radius = jnp.sqrt(column[j] * column[j] + column[j + 1] * column[j + 1])
        cosine = column[j] / radius
        sine_term = column[j + 1] / radius
        column[j] = radius
        cosines.append(cosine)
        sines.append(sine_term)
        targets[j + 1] = -sine_term * targets[j]
        targets[j] = cosine * targets[j]
        triangle.append(column[:j + 1])
    coeffs = [None] * total_steps
    for j in reversed(range(total_steps)):
        running = targets[j]
        for k in range(j + 1, total_steps):
            running = running - triangle[k][j] * coeffs[k]
        coeffs[j] = running / triangle[j][j]
    return jnp.stack(coeffs, axis=1)

def apply_matrix(vector, blocks, block_rows, block_cols, diagonal):
    systems = vector.shape[0]
    pieces = vector.reshape(systems, N_ROW, N_COL, PB * BS)
    tiled = blocks.reshape(TILES, CAP, BS, BS)

    def one_tile(accumulated, tile_index):
        row_index = tile_index // N_COL
        col_index = tile_index % N_COL
        column_group = lax.dynamic_index_in_dim(pieces, col_index, 2, keepdims=False)
        column_group = column_group.reshape(systems, N_ROW * PB, BS)
        picked = jnp.take(column_group, block_cols[tile_index].astype(jnp.int32), axis=1)
        tile_blocks = lax.dynamic_index_in_dim(tiled, tile_index, 0, keepdims=False)
        products = jnp.einsum('kij,nkj->nki', tile_blocks, picked, precision=lax.Precision.HIGHEST)
        row_sums = jax.ops.segment_sum(jnp.transpose(products, (1, 0, 2)), block_rows[tile_index].astype(jnp.int32), num_segments=N_COL * PB)
        partial_value = jnp.transpose(row_sums, (1, 0, 2)).reshape(systems, N_COL * PB * BS)
        accumulated = accumulated.at[:, row_index].add(partial_value)
        return (accumulated, None)
    start = jnp.zeros((systems, N_ROW, N_COL * PB * BS), jnp.float32)
    accumulated, unused = lax.scan(one_tile, start, jnp.arange(TILES, dtype=jnp.int32))
    return diagonal[None, :] * vector + accumulated.reshape(systems, -1)

def reference(blocks, block_rows, block_cols, diagonal, right_sides):
    systems = right_sides.shape[0]
    initial_norm = jnp.sqrt(lax.optimization_barrier(jnp.sum(right_sides * right_sides, axis=1)) + epsilon)
    krylov_basis = [right_sides / initial_norm[:, None]]
    hessenberg = jnp.zeros((systems, STEPS + 1, STEPS), jnp.float32)
    for j in range(STEPS):
        candidate = apply_matrix(krylov_basis[j], blocks, block_rows, block_cols, diagonal)
        stacked = jnp.stack(krylov_basis)
        coeffs = jnp.einsum('inl,nl->ni', stacked, candidate, precision=lax.Precision.HIGHEST)
        candidate = candidate - jnp.einsum('ni,inl->nl', coeffs, stacked, precision=lax.Precision.HIGHEST)
        new_norm = jnp.sqrt(lax.optimization_barrier(jnp.sum(candidate * candidate, axis=1)) + epsilon)
        hessenberg = hessenberg.at[:, :j + 1, j].set(coeffs)
        hessenberg = hessenberg.at[:, j + 1, j].set(new_norm)
        krylov_basis.append(candidate / new_norm[:, None])
    weights = least_squares(hessenberg, initial_norm)
    solution = jnp.einsum('ni,inl->nl', weights, jnp.stack(krylov_basis[:STEPS]), precision=lax.Precision.HIGHEST)
    return (solution, hessenberg)
```

```python
import functools

import jax
import jax.numpy as jnp
from jax import lax
from jax.experimental import pallas as pl
from jax.experimental.pallas import tpu as pltpu
from jax.sharding import PartitionSpec as P

STEPS = 8
SLOTS = 24

epsilon = 1e-06
MESH = pl.DeviceIdType.MESH
f32 = jnp.float32
bf16 = jnp.bfloat16


def exact_pick(onehot, values):
    high = values.astype(bf16)
    low = (values - high.astype(f32)).astype(bf16)
    return jnp.dot(onehot, high, preferred_element_type=f32) + jnp.dot(
        onehot, low, preferred_element_type=f32
    )


def kernel(
    n_row, n_col, slots,
    pos_ref, rowof_ref, cols_ref, diag_ref, rhs_ref, blocks_ref,
    sol_ref, hess_ref,
    staged, weights, pick, compact, spread,
    basis, picked_basis, u_ref, pu_ref, y_ref, base_ref,
    gathered, sums_out, sums_in, dots1, dots2, norm1, norm2,
    load_sem, ag_send, ag_recv, rs_send, rs_recv,
    d1_send, d1_recv, d2_send, d2_recv, n1_send, n1_recv, n2_send, n2_recv,
):
    me_r, me_c = lax.axis_index("row"), lax.axis_index("col")
    systems, piece, width = rhs_ref.shape
    cap = blocks_ref.shape[0]
    part = 128 // systems

    def load(t):
        return pltpu.make_async_copy(
            blocks_ref.at[pl.ds(t * 8, 8)], staged.at[pl.ds(t * 8, 8)], load_sem.at[t]
        )

    def start_load(t, carry):
        load(t).start()
        return carry

    lax.fori_loop(0, cap // 8, start_load, 0)

    row_peers = [lax.rem(me_r + d, n_row) for d in range(1, n_row)]
    col_peers = [lax.rem(me_c + d, n_col) for d in range(1, n_col)]

    barrier = pltpu.get_barrier_semaphore()
    for peer in row_peers:
        pl.semaphore_signal(barrier, inc=1, device_id=(peer, me_c), device_id_type=MESH)
    for peer in col_peers:
        pl.semaphore_signal(barrier, inc=1, device_id=(me_r, peer), device_id_type=MESH)

    def shared(buffer, send_sem, recv_sem, axis):
        if axis == "row":
            peers, me = row_peers, me_r
        else:
            peers, me = col_peers, me_c

        def copy(peer, slot):
            return pltpu.make_async_remote_copy(
                src_ref=buffer.at[slot],
                dst_ref=buffer.at[slot],
                send_sem=send_sem.at[peer],
                recv_sem=recv_sem.at[slot],
                device_id=(peer, me_c) if axis == "row" else (me_r, peer),
                device_id_type=MESH,
            )

        def start():
            for peer in peers:
                copy(peer, me).start()

        def receive(peer):
            copy(peer, peer).wait_recv()

        def receive_all():
            for peer in peers:
                receive(peer)

        def finish():
            for peer in peers:
                copy(peer, me).wait_send()

        return start, receive, receive_all, finish

    def gather_of(parity):
        return shared(gathered.at[parity], ag_send.at[parity], ag_recv.at[parity], "row")

    n1_start, _, n1_receive, n1_finish = shared(norm1, n1_send, n1_recv, "col")
    n2_start, _, n2_receive, n2_finish = shared(norm2, n2_send, n2_recv, "row")
    d1_start, _, d1_receive, d1_finish = shared(dots1, d1_send, d1_recv, "col")
    d2_start, _, d2_receive, d2_finish = shared(dots2, d2_send, d2_recv, "row")

    def sums_copy(peer, source, target):
        return pltpu.make_async_remote_copy(
            src_ref=sums_out.at[source],
            dst_ref=sums_in.at[target],
            send_sem=rs_send.at[peer],
            recv_sem=rs_recv.at[target],
            device_id=(me_r, peer),
            device_id_type=MESH,
        )

    lane_part = lax.broadcasted_iota(jnp.int32, (8, 128), 1) // part

    def fold(x):
        out = jnp.zeros((8, 128), f32)
        for n in range(systems):
            total = jnp.sum(x[:, n * width : (n + 1) * width], axis=1, keepdims=True)
            out = jnp.where(lane_part == n, total, out)
        return out

    def unfold(row):
        return jnp.concatenate(
            [
                jnp.broadcast_to(row[:, n * part : n * part + 1], (1, width))
                for n in range(systems)
            ],
            axis=1,
        )

    def sum_rows(x):
        return jnp.sum(x, axis=0, keepdims=True)

    def send_norm(u):
        squares = sum_rows(u * u)
        norm1[me_c] = fold(jnp.broadcast_to(squares, (8, systems * width)))
        n1_start()

    def relay_norm():
        n1_receive()
        norm2[me_r] = jnp.sum(norm1[...], axis=0)
        n2_start()

    def take_norm():
        n2_receive()
        total = jnp.sum(norm2[...], axis=0)
        n1_finish()
        n2_finish()
        return jnp.sqrt(total + epsilon)

    pl.semaphore_wait(barrier, n_row - 1 + n_col - 1)

    u = jnp.concatenate([rhs_ref[n] for n in range(systems)], axis=1)
    u_ref[...] = u
    gathered[0, me_r] = u
    start, receive, receive_all, finish = gather_of(0)
    start()
    send_norm(u)

    basis[...] = jnp.zeros_like(basis)
    picked_basis[...] = jnp.zeros_like(picked_basis)

    def onehot(index, shape, axis):
        hit = index == lax.broadcasted_iota(jnp.int32, shape, axis)
        return jnp.where(hit, 1.0, 0.0).astype(bf16)

    for r in range(n_row):
        pick[r] = onehot(cols_ref[...] - r * piece, (cap, piece), 1)
    compact[...] = onehot(pos_ref[...], (n_col * slots, cap), 0)
    spread[...] = onehot(rowof_ref[...], (piece, n_col * slots), 0)

    def place(t, carry):
        load(t).wait()
        for r in range(8):
            half, kk, nn = r // 4, (r // 2) % 2, r % 2
            weights[
                2 * t + half, nn * width : (nn + 1) * width, kk * width : (kk + 1) * width
            ] = staged[8 * t + r].astype(bf16)
        return carry

    lax.fori_loop(0, cap // 8, place, 0)

    pu_ref[...] = exact_pick(pick[me_r], gathered[0, me_r])
    for peer in row_peers:
        receive(peer)
        pu_ref[...] += exact_pick(pick[peer], gathered[0, peer])
    finish()

    place_row = lax.broadcasted_iota(jnp.int32, (8, width), 0)
    second_k = (place_row // 2) % 2 == 1
    second_n = place_row % 2 == 1
    second_half = lax.broadcasted_iota(jnp.int32, (8, 2 * width), 0) // 4 == 1
    NT = (((1,), (1,)), ((), ()))
    group = 4 if cap % 32 == 0 else 1

    def products(s, carry):
        for inner in range(group):
            t = s * group + inner
            at = pl.ds(pl.multiple_of(8 * t, 8), 8)
            slab = pu_ref[at, :]
            lhs = []
            for n in range(systems):
                x = slab[:, n * width : (n + 1) * width]
                lhs.append(
                    jnp.concatenate(
                        [jnp.where(second_k, 0.0, x), jnp.where(second_k, x, 0.0)], axis=1
                    )
                )
            lhs = jnp.concatenate(lhs, axis=0).astype(bf16)
            first = lax.dot_general(lhs, weights[2 * t], NT, preferred_element_type=f32)
            second = lax.dot_general(lhs, weights[2 * t + 1], NT, preferred_element_type=f32)
            for n in range(systems):
                both = jnp.where(
                    second_half, second[8 * n : 8 * n + 8], first[8 * n : 8 * n + 8]
                )
                y_ref[at, n * width : (n + 1) * width] = jnp.where(
                    second_n, both[:, width:], both[:, :width]
                )
        return carry

    def arnoldi(j, carry):
        parity = lax.rem(j + 1, 2)
        start, receive, receive_all, finish = gather_of(parity)

        lax.fori_loop(0, cap // 8 // group, products, 0)
        packed = exact_pick(compact[...], y_ref[...])
        for c in range(n_col):
            sums_out[c] = packed[c * slots : (c + 1) * slots]
        for peer in col_peers:
            sums_copy(peer, peer, me_c).start()
        sums_in[me_c] = sums_out[me_c]

        relay_norm()
        norm = take_norm()
        hess_ref[j, 8:16, :] = norm
        inverse = unfold(1.0 / norm[0:1])
        v = u_ref[...] * inverse
        basis[j] = v
        picked_basis[j] = pu_ref[...] * inverse
        diag = diag_ref[...]
        base_ref[...] = jnp.concatenate([diag] * systems, axis=1) * v

        for peer in col_peers:
            sums_copy(peer, peer, peer).wait_recv()
        sums = jnp.concatenate([sums_in[c] for c in range(n_col)], axis=0)
        w = base_ref[...] + exact_pick(spread[...], sums) * inverse
        gathered[parity, me_r] = w
        start()

        rows = [sum_rows(basis[i] * w) for i in range(STEPS)]
        dots1[me_c] = fold(jnp.concatenate(rows, axis=0))
        d1_start()
        pu_ref[...] = exact_pick(pick[me_r], w)
        d1_receive()
        dots2[me_r] = jnp.sum(dots1[...], axis=0)
        d2_start()
        for peer in row_peers:
            receive(peer)
            pu_ref[...] += exact_pick(pick[peer], gathered[parity, peer])
        d2_receive()
        h = jnp.sum(dots2[...], axis=0)
        hess_ref[j, 0:8, :] = h
        factors = [unfold(h[i : i + 1]) for i in range(STEPS)]
        rest = gathered[parity, me_r]
        for i in range(STEPS):
            rest = rest - factors[i] * basis[i]
        u_ref[...] = rest
        send_norm(rest)
        picked = pu_ref[...]
        for i in range(STEPS):
            picked = picked - factors[i] * picked_basis[i]
        pu_ref[...] = picked

        for peer in col_peers:
            sums_copy(peer, peer, me_c).wait_send()
        finish()
        d1_finish()
        d2_finish()
        return carry

    lax.fori_loop(0, STEPS, arnoldi, 0)
    relay_norm()
    hess_ref[STEPS, 8:16, :] = take_norm()
    hess_ref[STEPS, 0:8, :] = jnp.zeros((8, 128), f32)

    initial = hess_ref[0, 8:9, :]
    targets = [initial] + [jnp.zeros_like(initial)] * STEPS
    cosines, sines, triangle = [], [], []
    for j in range(STEPS):
        column = [hess_ref[j, i : i + 1, :] for i in range(j + 1)]
        column.append(hess_ref[j + 1, 8:9, :])
        for i in range(j):
            leading, trailing = column[i], column[i + 1]
            column[i] = cosines[i] * leading + sines[i] * trailing
            column[i + 1] = cosines[i] * trailing - sines[i] * leading
        radius = jnp.sqrt(column[j] * column[j] + column[j + 1] * column[j + 1])
        cosine = column[j] / radius
        sine_term = column[j + 1] / radius
        column[j] = radius
        cosines.append(cosine)
        sines.append(sine_term)
        targets[j + 1] = -sine_term * targets[j]
        targets[j] = cosine * targets[j]
        triangle.append(column[: j + 1])
    coeffs = [None] * STEPS
    for j in reversed(range(STEPS)):
        running = targets[j]
        for k in range(j + 1, STEPS):
            running = running - triangle[k][j] * coeffs[k]
        coeffs[j] = running / triangle[j][j]
    result = unfold(coeffs[0]) * basis[0]
    for i in range(1, STEPS):
        result = result + unfold(coeffs[i]) * basis[i]
    for n in range(systems):
        sol_ref[n] = result[:, n * width : (n + 1) * width]


def run(n_row, n_col, slots, collective_id, pos, rowof, cols, diag, rhs, blocks):
    systems, piece, width = rhs.shape
    cap = blocks.shape[0]
    lanes = systems * width
    dma = pltpu.SemaphoreType.DMA
    vmem = pl.BlockSpec(memory_space=pltpu.VMEM)
    return pl.pallas_call(
        functools.partial(kernel, n_row, n_col, slots),
        out_shape=(
            jax.ShapeDtypeStruct((systems, piece, width), f32),
            jax.ShapeDtypeStruct((STEPS + 1, 16, 128), f32),
        ),
        in_specs=[vmem] * 5 + [pl.BlockSpec(memory_space=pl.ANY)],
        out_specs=(vmem, vmem),
        scratch_shapes=[
            pltpu.VMEM((cap, width, width), f32),
            pltpu.VMEM((cap // 4, 2 * width, 2 * width), bf16),
            pltpu.VMEM((n_row, cap, piece), bf16),
            pltpu.VMEM((n_col * slots, cap), bf16),
            pltpu.VMEM((piece, n_col * slots), bf16),
            pltpu.VMEM((STEPS, piece, lanes), f32),
            pltpu.VMEM((STEPS, cap, lanes), f32),
            pltpu.VMEM((piece, lanes), f32),
            pltpu.VMEM((cap, lanes), f32),
            pltpu.VMEM((cap, lanes), f32),
            pltpu.VMEM((piece, lanes), f32),
            pltpu.VMEM((2, n_row, piece, lanes), f32),
            pltpu.VMEM((n_col, slots, lanes), f32),
            pltpu.VMEM((n_col, slots, lanes), f32),
            pltpu.VMEM((n_col, 8, 128), f32),
            pltpu.VMEM((n_row, 8, 128), f32),
            pltpu.VMEM((n_col, 8, 128), f32),
            pltpu.VMEM((n_row, 8, 128), f32),
            dma((cap // 8,)),
            dma((2, n_row)),
            dma((2, n_row)),
            dma((n_col,)),
            dma((n_col,)),
            dma((n_col,)),
            dma((n_col,)),
            dma((n_row,)),
            dma((n_row,)),
            dma((n_col,)),
            dma((n_col,)),
            dma((n_row,)),
            dma((n_row,)),
        ],
        compiler_params=pltpu.CompilerParams(
            collective_id=collective_id,
            has_side_effects=True,
            vmem_limit_bytes=60000 * 1024,
        ),
    )(pos, rowof, cols, diag, rhs, blocks)


def body(n_row, n_col, blocks, block_rows, block_cols, diagonal, right_sides):
    systems = right_sides.shape[0]
    width = blocks.shape[1]
    cap = blocks.shape[0]
    piece = right_sides.shape[1] // width
    me_r, me_c = lax.axis_index("row"), lax.axis_index("col")

    all_rows = lax.all_gather(block_rows, ("row", "col"), axis=0, tiled=True)
    first = jnp.concatenate(
        [jnp.ones_like(all_rows[:, :1], bool), all_rows[:, 1:] != all_rows[:, :-1]], axis=1
    )
    pieces = all_rows // piece
    order = jnp.arange(cap, dtype=jnp.int32)
    earlier = order[None, :, None] >= order[None, None, :]
    same = pieces[:, :, None] == pieces[:, None, :]
    rank = (
        jnp.sum((earlier & same & first[:, None, :]).astype(jnp.int32), axis=2) - 1
    )

    group = lambda a: lax.dynamic_slice_in_dim(a, me_r * n_col, n_col, 0)
    g_rows, g_pieces, g_rank = group(all_rows), group(pieces), group(rank)
    own = lambda a: lax.dynamic_slice_in_dim(a, me_c, 1, 0)

    cols = block_cols.reshape(cap, 1)
    diag = diagonal.reshape(piece, width)
    rhs = right_sides.reshape(systems, piece, width)

    def path(slots, collective_id):
        def call(g_rows, g_pieces, g_rank, cols, diag, rhs, blocks):
            pos = own(g_pieces) * slots + own(g_rank)
            slot = jnp.arange(slots, dtype=jnp.int32)
            hit = (g_pieces == me_c)[:, None, :] & (g_rank[:, None, :] == slot[None, :, None])
            rowof = jnp.max(jnp.where(hit, (g_rows % piece)[:, None, :], -1), axis=2)
            return run(
                n_row, n_col, slots, collective_id,
                pos, rowof.reshape(1, n_col * slots), cols, diag, rhs, blocks,
            )

        return call

    operands = (g_rows, g_pieces, g_rank, cols, diag, rhs, blocks)
    most = min(cap, piece)
    if SLOTS >= most:
        sol, hess = path(most, 0)(*operands)
    else:
        sol, hess = lax.cond(
            jnp.max(rank) < SLOTS, path(SLOTS, 0), path(most, 1), *operands
        )
    part = 128 // systems
    values = jnp.stack([hess[:, :, n * part] for n in range(systems)])
    upper = jnp.transpose(values[:, :STEPS, :STEPS], (0, 2, 1))
    upper = jnp.concatenate([upper, jnp.zeros((systems, 1, STEPS), f32)], axis=1)
    below = values[:, 1:, 8]
    i = jnp.arange(STEPS + 1)[:, None]
    j = jnp.arange(STEPS)[None, :]
    hessenberg = jnp.where(i <= j, upper, jnp.where(i == j + 1, below[:, None, :], 0.0))
    return sol.reshape(systems, piece * width), hessenberg


def solution(mesh):
    return jax.shard_map(
        functools.partial(body, mesh.shape["row"], mesh.shape["col"]),
        mesh=mesh,
        in_specs=(
            P(("row", "col"), None, None),
            P(("row", "col"), None),
            P(("row", "col"), None),
            P(("row", "col")),
            P(None, ("row", "col")),
        ),
        out_specs=(P(None, ("row", "col")), P()),
        check_vma=False,
    )
```

```python
import functools

import jax
import jax.numpy as jnp
from jax import lax
from jax.experimental import pallas as pl
from jax.experimental.pallas import tpu as pltpu
from jax.sharding import PartitionSpec as P

STEPS = 8
SLOTS = 24

epsilon = 1e-06
MESH = pl.DeviceIdType.MESH
f32 = jnp.float32
bf16 = jnp.bfloat16


def exact_pick(onehot, values):
    high = values.astype(bf16)
    low = (values - high.astype(f32)).astype(bf16)
    return jnp.dot(onehot, high, preferred_element_type=f32) + jnp.dot(
        onehot, low, preferred_element_type=f32
    )


def kernel(
    n_row, n_col, slots,
    pos_ref, rowof_ref, cols_ref, over_ref, diag_ref, rhs_ref, blocks_ref,
    sol_ref, hess_ref,
    staged, weights, pick, compact, spread,
    basis, picked_basis, u_ref, pu_ref, y_ref, base_ref, factor_ref,
    gathered, sums_out, sums_in, rowof_in, dots, norms,
    load_sem, ag_send, ag_recv, rs_send, rs_recv, ro_send, ro_recv,
    d_send, d_recv, n_send, n_recv,
):
    me_r, me_c = lax.axis_index("row"), lax.axis_index("col")
    systems = rhs_ref.shape[0]
    piece, width = diag_ref.shape
    cap = blocks_ref.shape[0]
    n_all = n_row * n_col
    me = me_r * n_col + me_c
    part = 128 // systems

    def load(t):
        return pltpu.make_async_copy(
            blocks_ref.at[pl.ds(t * 8, 8)], staged.at[pl.ds(t * 8, 8)], load_sem.at[t]
        )

    def start_load(t, carry):
        load(t).start()
        return carry

    lax.fori_loop(0, cap // 8, start_load, 0)

    row_peers = [lax.rem(me_r + d, n_row) for d in range(1, n_row)]
    col_peers = [lax.rem(me_c + d, n_col) for d in range(1, n_col)]

    def device(index):
        return (index // n_col, lax.rem(index, n_col))

    barrier = pltpu.get_barrier_semaphore()

    def greet(d, carry):
        pl.semaphore_signal(
            barrier, inc=1, device_id=device(lax.rem(me + d, n_all)), device_id_type=MESH
        )
        return carry

    lax.fori_loop(1, n_all, greet, 0)

    def remote(source, target, send_sem, recv_sem, peer):
        return pltpu.make_async_remote_copy(
            src_ref=source,
            dst_ref=target,
            send_sem=send_sem,
            recv_sem=recv_sem,
            device_id=peer,
            device_id_type=MESH,
        )

    def to_all(buffer, send_sem, recv_sem):
        def copy(peer, slot):
            at = buffer.at[slot]
            return remote(at, at, send_sem.at[peer], recv_sem.at[slot], device(peer))

        def each(act):
            def one(d, carry):
                act(lax.rem(me + d, n_all))
                return carry

            lax.fori_loop(1, n_all, one, 0)

        start = lambda: each(lambda peer: copy(peer, me).start())
        receive = lambda: each(lambda peer: copy(peer, peer).wait_recv())
        finish = lambda: each(lambda peer: copy(peer, me).wait_send())
        return start, receive, finish

    def gather_of(parity):
        def copy(peer, slot):
            at = gathered.at[parity, slot]
            return remote(
                at, at, ag_send.at[parity, peer], ag_recv.at[parity, slot], (peer, me_c)
            )

        def start():
            for peer in row_peers:
                copy(peer, me_r).start()

        def receive(peer):
            copy(peer, peer).wait_recv()

        def finish():
            for peer in row_peers:
                copy(peer, me_r).wait_send()

        return start, receive, finish

    n_start, n_receive, n_finish = to_all(norms, n_send, n_recv)
    d_start, d_receive, d_finish = to_all(dots, d_send, d_recv)

    def sums_copy(peer, source, target):
        return remote(
            sums_out.at[source], sums_in.at[target],
            rs_send.at[peer], rs_recv.at[target], (me_r, peer),
        )

    def rowof_copy(peer, source, target):
        return remote(
            rowof_ref.at[source], rowof_in.at[target],
            ro_send.at[peer], ro_recv.at[target], (me_r, peer),
        )

    lane_part = lax.broadcasted_iota(jnp.int32, (8, 128), 1) // part

    def fold(x):
        out = jnp.zeros((8, 128), f32)
        for n in range(systems):
            total = jnp.sum(x[:, n * width : (n + 1) * width], axis=1, keepdims=True)
            out = jnp.where(lane_part == n, total, out)
        return out

    def unfold(row):
        return jnp.concatenate(
            [
                jnp.broadcast_to(row[:, n * part : n * part + 1], (1, width))
                for n in range(systems)
            ],
            axis=1,
        )

    def sum_rows(x):
        return jnp.sum(x, axis=0, keepdims=True)

    def send_norm(u):
        squares = fold(jnp.broadcast_to(sum_rows(u * u), (8, systems * width)))
        second = lax.broadcasted_iota(jnp.int32, (8, 128), 0) == 1
        norms[me] = jnp.where(second, over_ref[...], squares)
        n_start()

    def take_norm():
        n_receive()
        total = jnp.sum(norms[...], axis=0)
        n_finish()
        return jnp.where(
            lax.broadcasted_iota(jnp.int32, (8, 128), 0) == 1, total, jnp.sqrt(total + epsilon)
        )

    for n in range(systems):
        for b in range(0, piece, 8):
            gathered[0, me_r, b : b + 8, n * width : (n + 1) * width] = jnp.concatenate(
                [
                    rhs_ref[n : n + 1, (b + r) * width : (b + r + 1) * width]
                    for r in range(8)
                ],
                axis=0,
            )
    pl.semaphore_wait(barrier, n_all - 1)
    start, receive, finish = gather_of(0)
    start()
    for peer in col_peers:
        rowof_copy(peer, peer, me_c).start()
    rowof_in[me_c] = rowof_ref[me_c]

    factor_ref[...] = jnp.zeros_like(factor_ref)
    basis[...] = jnp.zeros_like(basis)
    picked_basis[...] = jnp.zeros_like(picked_basis)

    def onehot(index, shape, axis):
        hit = index == lax.broadcasted_iota(jnp.int32, shape, axis)
        return jnp.where(hit, 1.0, 0.0).astype(bf16)

    cols = jnp.transpose(jnp.broadcast_to(cols_ref[...], (piece, cap)))
    for r in range(n_row):
        pick[r] = onehot(cols - r * piece, (cap, piece), 1)
    compact[...] = onehot(pos_ref[...], (n_col * slots, cap), 0)

    def place(t, carry):
        load(t).wait()
        for r in range(8):
            half, kk, nn = r // 4, (r // 2) % 2, r % 2
            weights[
                2 * t + half, nn * width : (nn + 1) * width, kk * width : (kk + 1) * width
            ] = staged[8 * t + r].astype(bf16)
        return carry

    lax.fori_loop(0, cap // 8, place, 0)

    pu_ref[...] = exact_pick(pick[me_r], gathered[0, me_r])
    for peer in row_peers:
        receive(peer)
        pu_ref[...] += exact_pick(pick[peer], gathered[0, peer])
    finish()
    for peer in col_peers:
        rowof_copy(peer, peer, peer).wait_recv()
    spread[...] = jnp.concatenate(
        [
            onehot(rowof_in[c, 0:1, :], (piece, rowof_in.shape[2]), 0)[:, :slots]
            for c in range(n_col)
        ],
        axis=1,
    )
    for peer in col_peers:
        rowof_copy(peer, peer, me_c).wait_send()

    place_row = lax.broadcasted_iota(jnp.int32, (8, width), 0)
    second_k = (place_row // 2) % 2 == 1
    second_n = place_row % 2 == 1
    second_half = lax.broadcasted_iota(jnp.int32, (8, 2 * width), 0) // 4 == 1
    NT = (((1,), (1,)), ((), ()))
    group = 4 if cap % 32 == 0 else 1

    def products(s, carry):
        for inner in range(group):
            t = s * group + inner
            at = pl.ds(pl.multiple_of(8 * t, 8), 8)
            slab = pu_ref[at, :]
            lhs = []
            for n in range(systems):
                x = slab[:, n * width : (n + 1) * width]
                lhs.append(
                    jnp.concatenate(
                        [jnp.where(second_k, 0.0, x), jnp.where(second_k, x, 0.0)], axis=1
                    )
                )
            lhs = jnp.concatenate(lhs, axis=0).astype(bf16)
            first = lax.dot_general(lhs, weights[2 * t], NT, preferred_element_type=f32)
            second = lax.dot_general(lhs, weights[2 * t + 1], NT, preferred_element_type=f32)
            for n in range(systems):
                both = jnp.where(
                    second_half, second[8 * n : 8 * n + 8], first[8 * n : 8 * n + 8]
                )
                y_ref[at, n * width : (n + 1) * width] = jnp.where(
                    second_n, both[:, width:], both[:, :width]
                )
        return carry

    def arnoldi(j, carry):
        parity = lax.rem(j + 1, 2)
        start, receive, finish = gather_of(parity)

        lax.fori_loop(0, cap // 8 // group, products, 0)
        packed = jnp.dot(
            compact[...], y_ref[...].astype(bf16), preferred_element_type=f32
        )
        for c in range(n_col):
            sums_out[c] = packed[c * slots : (c + 1) * slots]
        for peer in col_peers:
            sums_copy(peer, peer, me_c).start()
        sums_in[me_c] = sums_out[me_c]

        u = gathered[1 - parity, me_r]
        factors = [unfold(factor_ref[i : i + 1, :]) for i in range(STEPS)]
        for i in range(STEPS):
            u = u - factors[i] * basis[i]
        u_ref[...] = u
        send_norm(u)
        diag = diag_ref[...]
        base_ref[...] = jnp.concatenate([diag] * systems, axis=1) * u
        norm = take_norm()
        hess_ref[j, 8:16, :] = norm
        inverse = unfold(1.0 / norm[0:1])

        for peer in col_peers:
            sums_copy(peer, peer, peer).wait_recv()
        sums = jnp.concatenate([sums_in[c] for c in range(n_col)], axis=0)
        w = (
            base_ref[...]
            + jnp.dot(spread[...], sums.astype(bf16), preferred_element_type=f32)
        ) * inverse
        gathered[parity, me_r] = w
        start()

        basis[j] = u_ref[...] * inverse
        rows = [sum_rows(basis[i] * w) for i in range(STEPS)]
        dots[me] = fold(jnp.concatenate(rows, axis=0))
        d_start()
        picked_basis[j] = pu_ref[...] * inverse
        pu_ref[...] = exact_pick(pick[me_r], gathered[parity, me_r])
        for peer in row_peers:
            receive(peer)
            pu_ref[...] += exact_pick(pick[peer], gathered[parity, peer])
        d_receive()
        h = jnp.sum(dots[...], axis=0)
        hess_ref[j, 0:8, :] = h
        factor_ref[...] = h
        picked = pu_ref[...]
        for i in range(STEPS):
            picked = picked - unfold(h[i : i + 1]) * picked_basis[i]
        pu_ref[...] = picked

        for peer in col_peers:
            sums_copy(peer, peer, me_c).wait_send()
        finish()
        d_finish()
        return carry

    lax.fori_loop(0, STEPS, arnoldi, 0)
    u = gathered[STEPS % 2, me_r]
    for i in range(STEPS):
        u = u - unfold(factor_ref[i : i + 1, :]) * basis[i]
    send_norm(u)
    hess_ref[STEPS, 8:16, :] = take_norm()
    hess_ref[STEPS, 0:8, :] = jnp.zeros((8, 128), f32)

    initial = hess_ref[0, 8:9, :]
    targets = [initial] + [jnp.zeros_like(initial)] * STEPS
    cosines, sines, triangle = [], [], []
    for j in range(STEPS):
        column = [hess_ref[j, i : i + 1, :] for i in range(j + 1)]
        column.append(hess_ref[j + 1, 8:9, :])
        for i in range(j):
            leading, trailing = column[i], column[i + 1]
            column[i] = cosines[i] * leading + sines[i] * trailing
            column[i + 1] = cosines[i] * trailing - sines[i] * leading
        radius = jnp.sqrt(column[j] * column[j] + column[j + 1] * column[j + 1])
        cosine = column[j] / radius
        sine_term = column[j + 1] / radius
        column[j] = radius
        cosines.append(cosine)
        sines.append(sine_term)
        targets[j + 1] = -sine_term * targets[j]
        targets[j] = cosine * targets[j]
        triangle.append(column[: j + 1])
    coeffs = [None] * STEPS
    for j in reversed(range(STEPS)):
        running = targets[j]
        for k in range(j + 1, STEPS):
            running = running - triangle[k][j] * coeffs[k]
        coeffs[j] = running / triangle[j][j]
    result = unfold(coeffs[0]) * basis[0]
    for i in range(1, STEPS):
        result = result + unfold(coeffs[i]) * basis[i]
    for n in range(systems):
        sol_ref[n] = result[:, n * width : (n + 1) * width]


def run(n_row, n_col, slots, collective_id, pos, rowof, cols, over, diag, rhs, blocks):
    systems = rhs.shape[0]
    piece, width = diag.shape
    cap = blocks.shape[0]
    lanes = systems * width
    n_all = n_row * n_col
    dma = pltpu.SemaphoreType.DMA
    vmem = pl.BlockSpec(memory_space=pltpu.VMEM)
    return pl.pallas_call(
        functools.partial(kernel, n_row, n_col, slots),
        out_shape=(
            jax.ShapeDtypeStruct((systems, piece, width), f32),
            jax.ShapeDtypeStruct((STEPS + 1, 16, 128), f32),
        ),
        in_specs=[vmem] * 6 + [pl.BlockSpec(memory_space=pl.ANY)],
        out_specs=(vmem, vmem),
        scratch_shapes=[
            pltpu.VMEM((cap, width, width), f32),
            pltpu.VMEM((cap // 4, 2 * width, 2 * width), bf16),
            pltpu.VMEM((n_row, cap, piece), bf16),
            pltpu.VMEM((n_col * slots, cap), bf16),
            pltpu.VMEM((piece, n_col * slots), bf16),
            pltpu.VMEM((STEPS, piece, lanes), f32),
            pltpu.VMEM((STEPS, cap, lanes), f32),
            pltpu.VMEM((piece, lanes), f32),
            pltpu.VMEM((cap, lanes), f32),
            pltpu.VMEM((cap, lanes), f32),
            pltpu.VMEM((piece, lanes), f32),
            pltpu.VMEM((8, 128), f32),
            pltpu.VMEM((2, n_row, piece, lanes), f32),
            pltpu.VMEM((n_col, slots, lanes), f32),
            pltpu.VMEM((n_col, slots, lanes), f32),
            pltpu.VMEM(rowof.shape, jnp.int32),
            pltpu.VMEM((n_all, 8, 128), f32),
            pltpu.VMEM((n_all, 8, 128), f32),
            dma((cap // 8,)),
            dma((2, n_row)),
            dma((2, n_row)),
            dma((n_col,)),
            dma((n_col,)),
            dma((n_col,)),
            dma((n_col,)),
            dma((n_all,)),
            dma((n_all,)),
            dma((n_all,)),
            dma((n_all,)),
        ],
        compiler_params=pltpu.CompilerParams(
            collective_id=collective_id,
            has_side_effects=True,
            vmem_limit_bytes=60000 * 1024,
        ),
    )(pos, rowof, cols, over, diag, rhs, blocks)


def body(n_row, n_col, blocks, block_rows, block_cols, diagonal, right_sides):
    systems = right_sides.shape[0]
    width = blocks.shape[1]
    cap = blocks.shape[0]
    piece = right_sides.shape[1] // width

    rows = block_rows[0]
    first = jnp.concatenate([jnp.ones((1,), bool), rows[1:] != rows[:-1]])
    pieces = rows // piece
    order = jnp.arange(cap, dtype=jnp.int32)
    before = (order[:, None] >= order[None, :]) & (pieces[:, None] == pieces[None, :])
    rank = (
        jnp.sum((before & first[None, :]).astype(jnp.int32), axis=1) - 1
    )
    diag = diagonal.reshape(piece, width)

    def path(slots, collective_id):
        pos = (pieces * slots + rank)[None, :]
        columns = -(-slots // 128) * 128
        slot = jnp.arange(columns, dtype=jnp.int32)
        column = jnp.arange(n_col, dtype=jnp.int32)
        hit = (pieces == column[:, None])[:, None, :] & (
            rank[None, None, :] == slot[None, :, None]
        )
        rowof = jnp.max(jnp.where(hit, (rows % piece)[None, None, :], -1), axis=2)
        rowof = jnp.broadcast_to(rowof[:, None, :], (n_col, 8, columns))
        over = jnp.full((8, 128), jnp.where(jnp.max(rank) < slots, 0.0, 1.0), f32)
        return run(
            n_row, n_col, slots, collective_id,
            pos, rowof, block_cols, over, diag, right_sides, blocks,
        )

    most = min(cap, piece)
    sol, hess = path(min(SLOTS, most), 0)
    if SLOTS < most:
        sol, hess = lax.cond(
            hess[0, 9, 0] == 0.0, lambda s, h: (s, h), lambda s, h: path(most, 1), sol, hess
        )
    part = 128 // systems
    values = jnp.stack([hess[:, :, n * part] for n in range(systems)])
    upper = jnp.transpose(values[:, :STEPS, :STEPS], (0, 2, 1))
    upper = jnp.concatenate([upper, jnp.zeros((systems, 1, STEPS), f32)], axis=1)
    below = values[:, 1:, 8]
    i = jnp.arange(STEPS + 1)[:, None]
    j = jnp.arange(STEPS)[None, :]
    hessenberg = jnp.where(i <= j, upper, jnp.where(i == j + 1, below[:, None, :], 0.0))
    return sol.reshape(systems, piece * width), hessenberg


def solution(mesh):
    return jax.shard_map(
        functools.partial(body, mesh.shape["row"], mesh.shape["col"]),
        mesh=mesh,
        in_specs=(
            P(("row", "col"), None, None),
            P(("row", "col"), None),
            P(("row", "col"), None),
            P(("row", "col")),
            P(None, ("row", "col")),
        ),
        out_specs=(P(None, ("row", "col")), P()),
        check_vma=False,
    )
```

```python
import functools

import jax
import jax.numpy as jnp
from jax import lax
from jax.experimental import pallas as pl
from jax.experimental.pallas import tpu as pltpu
from jax.sharding import PartitionSpec as P

STEPS = 8
SLOTS = 24

epsilon = 1e-06
MESH = pl.DeviceIdType.MESH
f32 = jnp.float32
bf16 = jnp.bfloat16


def exact_pick(onehot, values):
    high = values.astype(bf16)
    low = (values - high.astype(f32)).astype(bf16)
    return jnp.dot(onehot, high, preferred_element_type=f32) + jnp.dot(
        onehot, low, preferred_element_type=f32
    )


def kernel(
    n_row, n_col, slots,
    pos_ref, rowof_ref, cols_ref, over_ref, diag_ref, rhs_ref, blocks_ref,
    sol_ref, hess_ref,
    staged, weights, pick, compact, spread,
    basis, picked_basis, u_ref, pu_ref, y_ref, base_ref, factor_ref,
    gathered, sums_out, sums_in, rowof_in, dots1, dots2, norms1, norms2,
    load_sem, ag_send, ag_recv, rs_send, rs_recv, ro_send, ro_recv,
    d1_send, d1_recv, d2_send, d2_recv, n1_send, n1_recv, n2_send, n2_recv,
):
    me_r, me_c = lax.axis_index("row"), lax.axis_index("col")
    systems = rhs_ref.shape[0]
    piece, width = diag_ref.shape
    cap = blocks_ref.shape[0]
    part = 128 // systems

    def load(t):
        return pltpu.make_async_copy(
            blocks_ref.at[pl.ds(t * 8, 8)], staged.at[pl.ds(t * 8, 8)], load_sem.at[t]
        )

    def start_load(t, carry):
        load(t).start()
        return carry

    lax.fori_loop(0, cap // 8, start_load, 0)

    row_peers = [lax.rem(me_r + d, n_row) for d in range(1, n_row)]
    col_peers = [lax.rem(me_c + d, n_col) for d in range(1, n_col)]

    barrier = pltpu.get_barrier_semaphore()
    for peer in row_peers:
        pl.semaphore_signal(barrier, inc=1, device_id=(peer, me_c), device_id_type=MESH)
    for peer in col_peers:
        pl.semaphore_signal(barrier, inc=1, device_id=(me_r, peer), device_id_type=MESH)

    def remote(source, target, send_sem, recv_sem, peer):
        return pltpu.make_async_remote_copy(
            src_ref=source,
            dst_ref=target,
            send_sem=send_sem,
            recv_sem=recv_sem,
            device_id=peer,
            device_id_type=MESH,
        )

    def two_stage(first, second, send1, recv1, send2, recv2):
        def along_col(peer, slot):
            at = first.at[slot]
            return remote(at, at, send1.at[peer], recv1.at[slot], (me_r, peer))

        def along_row(peer, slot):
            at = second.at[slot]
            return remote(at, at, send2.at[peer], recv2.at[slot], (peer, me_c))

        def start(value):
            first[me_c] = value
            for peer in col_peers:
                along_col(peer, me_c).start()

        def relay():
            for peer in col_peers:
                along_col(peer, peer).wait_recv()
            second[me_r] = jnp.sum(first[...], axis=0)
            for peer in row_peers:
                along_row(peer, me_r).start()

        def receive():
            for peer in row_peers:
                along_row(peer, peer).wait_recv()
            return jnp.sum(second[...], axis=0)

        def finish():
            for peer in col_peers:
                along_col(peer, me_c).wait_send()
            for peer in row_peers:
                along_row(peer, me_r).wait_send()

        return start, relay, receive, finish

    def gather_of(parity):
        def copy(peer, slot):
            at = gathered.at[parity, slot]
            return remote(
                at, at, ag_send.at[parity, peer], ag_recv.at[parity, slot], (peer, me_c)
            )

        def start():
            for peer in row_peers:
                copy(peer, me_r).start()

        def receive(peer):
            copy(peer, peer).wait_recv()

        def finish():
            for peer in row_peers:
                copy(peer, me_r).wait_send()

        return start, receive, finish

    n_start, n_relay, n_receive, n_finish = two_stage(
        norms1, norms2, n1_send, n1_recv, n2_send, n2_recv
    )
    d_start, d_relay, d_receive, d_finish = two_stage(
        dots1, dots2, d1_send, d1_recv, d2_send, d2_recv
    )

    def sums_copy(peer, source, target):
        return remote(
            sums_out.at[source], sums_in.at[target],
            rs_send.at[peer], rs_recv.at[target], (me_r, peer),
        )

    def rowof_copy(peer, source, target):
        return remote(
            rowof_ref.at[source], rowof_in.at[target],
            ro_send.at[peer], ro_recv.at[target], (me_r, peer),
        )

    lane_part = lax.broadcasted_iota(jnp.int32, (8, 128), 1) // part

    def fold(x):
        out = jnp.zeros((8, 128), f32)
        for n in range(systems):
            total = jnp.sum(x[:, n * width : (n + 1) * width], axis=1, keepdims=True)
            out = jnp.where(lane_part == n, total, out)
        return out

    def unfold(row):
        return jnp.concatenate(
            [
                jnp.broadcast_to(row[:, n * part : n * part + 1], (1, width))
                for n in range(systems)
            ],
            axis=1,
        )

    def sum_rows(x):
        return jnp.sum(x, axis=0, keepdims=True)

    def send_norm(u):
        squares = fold(jnp.broadcast_to(sum_rows(u * u), (8, systems * width)))
        second = lax.broadcasted_iota(jnp.int32, (8, 128), 0) == 1
        n_start(jnp.where(second, over_ref[...], squares))

    def take_norm():
        n_relay()
        total = n_receive()
        n_finish()
        return jnp.where(
            lax.broadcasted_iota(jnp.int32, (8, 128), 0) == 1, total, jnp.sqrt(total + epsilon)
        )

    for n in range(systems):
        for b in range(0, piece, 8):
            gathered[0, me_r, b : b + 8, n * width : (n + 1) * width] = jnp.concatenate(
                [
                    rhs_ref[n : n + 1, (b + r) * width : (b + r + 1) * width]
                    for r in range(8)
                ],
                axis=0,
            )
    pl.semaphore_wait(barrier, n_row - 1 + n_col - 1)
    start, receive, finish = gather_of(0)
    start()
    for peer in col_peers:
        rowof_copy(peer, peer, me_c).start()
    rowof_in[me_c] = rowof_ref[me_c]

    factor_ref[...] = jnp.zeros_like(factor_ref)
    basis[...] = jnp.zeros_like(basis)
    picked_basis[...] = jnp.zeros_like(picked_basis)

    def onehot(index, shape, axis):
        hit = index == lax.broadcasted_iota(jnp.int32, shape, axis)
        return jnp.where(hit, 1.0, 0.0).astype(bf16)

    cols = jnp.transpose(jnp.broadcast_to(cols_ref[...], (piece, cap)))
    for r in range(n_row):
        pick[r] = onehot(cols - r * piece, (cap, piece), 1)
    compact[...] = onehot(pos_ref[...], (n_col * slots, cap), 0)

    def place(t, carry):
        load(t).wait()
        for r in range(8):
            half, kk, nn = r // 4, (r // 2) % 2, r % 2
            weights[
                2 * t + half, nn * width : (nn + 1) * width, kk * width : (kk + 1) * width
            ] = staged[8 * t + r].astype(bf16)
        return carry

    lax.fori_loop(0, cap // 8, place, 0)

    pu_ref[...] = exact_pick(pick[me_r], gathered[0, me_r])
    for peer in row_peers:
        receive(peer)
        pu_ref[...] += exact_pick(pick[peer], gathered[0, peer])
    finish()
    for peer in col_peers:
        rowof_copy(peer, peer, peer).wait_recv()
    spread[...] = jnp.concatenate(
        [
            onehot(rowof_in[c, 0:1, :], (piece, rowof_in.shape[2]), 0)[:, :slots]
            for c in range(n_col)
        ],
        axis=1,
    )
    for peer in col_peers:
        rowof_copy(peer, peer, me_c).wait_send()

    place_row = lax.broadcasted_iota(jnp.int32, (8, width), 0)
    second_k = (place_row // 2) % 2 == 1
    second_n = place_row % 2 == 1
    second_half = lax.broadcasted_iota(jnp.int32, (8, 2 * width), 0) // 4 == 1
    NT = (((1,), (1,)), ((), ()))
    group = 4 if cap % 32 == 0 else 1

    def products(s, carry):
        for inner in range(group):
            t = s * group + inner
            at = pl.ds(pl.multiple_of(8 * t, 8), 8)
            slab = pu_ref[at, :]
            lhs = []
            for n in range(systems):
                x = slab[:, n * width : (n + 1) * width]
                lhs.append(
                    jnp.concatenate(
                        [jnp.where(second_k, 0.0, x), jnp.where(second_k, x, 0.0)], axis=1
                    )
                )
            lhs = jnp.concatenate(lhs, axis=0).astype(bf16)
            first = lax.dot_general(lhs, weights[2 * t], NT, preferred_element_type=f32)
            second = lax.dot_general(lhs, weights[2 * t + 1], NT, preferred_element_type=f32)
            for n in range(systems):
                both = jnp.where(
                    second_half, second[8 * n : 8 * n + 8], first[8 * n : 8 * n + 8]
                )
                y_ref[at, n * width : (n + 1) * width] = jnp.where(
                    second_n, both[:, width:], both[:, :width]
                )
        return carry

    def arnoldi(j, carry):
        parity = lax.rem(j + 1, 2)
        start, receive, finish = gather_of(parity)

        lax.fori_loop(0, cap // 8 // group, products, 0)
        packed = jnp.dot(
            compact[...], y_ref[...].astype(bf16), preferred_element_type=f32
        )
        for c in range(n_col):
            sums_out[c] = packed[c * slots : (c + 1) * slots]
        for peer in col_peers:
            sums_copy(peer, peer, me_c).start()
        sums_in[me_c] = sums_out[me_c]

        u = gathered[1 - parity, me_r]
        factors = [unfold(factor_ref[i : i + 1, :]) for i in range(STEPS)]
        for i in range(STEPS):
            u = u - factors[i] * basis[i]
        u_ref[...] = u
        send_norm(u)
        diag = diag_ref[...]
        base_ref[...] = jnp.concatenate([diag] * systems, axis=1) * u
        norm = take_norm()
        hess_ref[j, 8:16, :] = norm
        inverse = unfold(1.0 / norm[0:1])

        for peer in col_peers:
            sums_copy(peer, peer, peer).wait_recv()
        sums = jnp.concatenate([sums_in[c] for c in range(n_col)], axis=0)
        w = (
            base_ref[...]
            + jnp.dot(spread[...], sums.astype(bf16), preferred_element_type=f32)
        ) * inverse
        gathered[parity, me_r] = w
        start()

        basis[j] = u_ref[...] * inverse
        rows = [sum_rows(basis[i] * w) for i in range(STEPS)]
        d_start(fold(jnp.concatenate(rows, axis=0)))
        picked_basis[j] = pu_ref[...] * inverse
        pu_ref[...] = exact_pick(pick[me_r], gathered[parity, me_r])
        d_relay()
        for peer in row_peers:
            receive(peer)
            pu_ref[...] += exact_pick(pick[peer], gathered[parity, peer])
        h = d_receive()
        hess_ref[j, 0:8, :] = h
        factor_ref[...] = h
        picked = pu_ref[...]
        for i in range(STEPS):
            picked = picked - unfold(h[i : i + 1]) * picked_basis[i]
        pu_ref[...] = picked

        for peer in col_peers:
            sums_copy(peer, peer, me_c).wait_send()
        finish()
        d_finish()
        return carry

    lax.fori_loop(0, STEPS, arnoldi, 0)
    u = gathered[STEPS % 2, me_r]
    for i in range(STEPS):
        u = u - unfold(factor_ref[i : i + 1, :]) * basis[i]
    send_norm(u)
    hess_ref[STEPS, 8:16, :] = take_norm()
    hess_ref[STEPS, 0:8, :] = jnp.zeros((8, 128), f32)

    initial = hess_ref[0, 8:9, :]
    targets = [initial] + [jnp.zeros_like(initial)] * STEPS
    cosines, sines, triangle = [], [], []
    for j in range(STEPS):
        column = [hess_ref[j, i : i + 1, :] for i in range(j + 1)]
        column.append(hess_ref[j + 1, 8:9, :])
        for i in range(j):
            leading, trailing = column[i], column[i + 1]
            column[i] = cosines[i] * leading + sines[i] * trailing
            column[i + 1] = cosines[i] * trailing - sines[i] * leading
        radius = jnp.sqrt(column[j] * column[j] + column[j + 1] * column[j + 1])
        cosine = column[j] / radius
        sine_term = column[j + 1] / radius
        column[j] = radius
        cosines.append(cosine)
        sines.append(sine_term)
        targets[j + 1] = -sine_term * targets[j]
        targets[j] = cosine * targets[j]
        triangle.append(column[: j + 1])
    coeffs = [None] * STEPS
    for j in reversed(range(STEPS)):
        running = targets[j]
        for k in range(j + 1, STEPS):
            running = running - triangle[k][j] * coeffs[k]
        coeffs[j] = running / triangle[j][j]
    result = unfold(coeffs[0]) * basis[0]
    for i in range(1, STEPS):
        result = result + unfold(coeffs[i]) * basis[i]
    for n in range(systems):
        sol_ref[n] = result[:, n * width : (n + 1) * width]


def run(n_row, n_col, slots, collective_id, pos, rowof, cols, over, diag, rhs, blocks):
    systems = rhs.shape[0]
    piece, width = diag.shape
    cap = blocks.shape[0]
    lanes = systems * width
    dma = pltpu.SemaphoreType.DMA
    vmem = pl.BlockSpec(memory_space=pltpu.VMEM)
    return pl.pallas_call(
        functools.partial(kernel, n_row, n_col, slots),
        out_shape=(
            jax.ShapeDtypeStruct((systems, piece, width), f32),
            jax.ShapeDtypeStruct((STEPS + 1, 16, 128), f32),
        ),
        in_specs=[vmem] * 6 + [pl.BlockSpec(memory_space=pl.ANY)],
        out_specs=(vmem, vmem),
        scratch_shapes=[
            pltpu.VMEM((cap, width, width), f32),
            pltpu.VMEM((cap // 4, 2 * width, 2 * width), bf16),
            pltpu.VMEM((n_row, cap, piece), bf16),
            pltpu.VMEM((n_col * slots, cap), bf16),
            pltpu.VMEM((piece, n_col * slots), bf16),
            pltpu.VMEM((STEPS, piece, lanes), f32),
            pltpu.VMEM((STEPS, cap, lanes), f32),
            pltpu.VMEM((piece, lanes), f32),
            pltpu.VMEM((cap, lanes), f32),
            pltpu.VMEM((cap, lanes), f32),
            pltpu.VMEM((piece, lanes), f32),
            pltpu.VMEM((8, 128), f32),
            pltpu.VMEM((2, n_row, piece, lanes), f32),
            pltpu.VMEM((n_col, slots, lanes), f32),
            pltpu.VMEM((n_col, slots, lanes), f32),
            pltpu.VMEM(rowof.shape, jnp.int32),
            pltpu.VMEM((n_col, 8, 128), f32),
            pltpu.VMEM((n_row, 8, 128), f32),
            pltpu.VMEM((n_col, 8, 128), f32),
            pltpu.VMEM((n_row, 8, 128), f32),
            dma((cap // 8,)),
            dma((2, n_row)),
            dma((2, n_row)),
            dma((n_col,)),
            dma((n_col,)),
            dma((n_col,)),
            dma((n_col,)),
            dma((n_col,)),
            dma((n_col,)),
            dma((n_row,)),
            dma((n_row,)),
            dma((n_col,)),
            dma((n_col,)),
            dma((n_row,)),
            dma((n_row,)),
        ],
        compiler_params=pltpu.CompilerParams(
            collective_id=collective_id,
            has_side_effects=True,
            vmem_limit_bytes=60000 * 1024,
        ),
    )(pos, rowof, cols, over, diag, rhs, blocks)


def body(n_row, n_col, blocks, block_rows, block_cols, diagonal, right_sides):
    systems = right_sides.shape[0]
    width = blocks.shape[1]
    cap = blocks.shape[0]
    piece = right_sides.shape[1] // width

    rows = block_rows[0]
    first = jnp.concatenate([jnp.ones((1,), bool), rows[1:] != rows[:-1]])
    pieces = rows // piece
    order = jnp.arange(cap, dtype=jnp.int32)
    before = (order[:, None] >= order[None, :]) & (pieces[:, None] == pieces[None, :])
    rank = (
        jnp.sum((before & first[None, :]).astype(jnp.int32), axis=1) - 1
    )
    diag = diagonal.reshape(piece, width)

    def path(slots, collective_id):
        pos = (pieces * slots + rank)[None, :]
        columns = -(-slots // 128) * 128
        slot = jnp.arange(columns, dtype=jnp.int32)
        column = jnp.arange(n_col, dtype=jnp.int32)
        hit = (pieces == column[:, None])[:, None, :] & (
            rank[None, None, :] == slot[None, :, None]
        )
        rowof = jnp.max(jnp.where(hit, (rows % piece)[None, None, :], -1), axis=2)
        rowof = jnp.broadcast_to(rowof[:, None, :], (n_col, 8, columns))
        over = jnp.full((8, 128), jnp.where(jnp.max(rank) < slots, 0.0, 1.0), f32)
        return run(
            n_row, n_col, slots, collective_id,
            pos, rowof, block_cols, over, diag, right_sides, blocks,
        )

    most = min(cap, piece)
    sol, hess = path(min(SLOTS, most), 0)
    if SLOTS < most:
        sol, hess = lax.cond(
            hess[0, 9, 0] == 0.0, lambda s, h: (s, h), lambda s, h: path(most, 1), sol, hess
        )
    part = 128 // systems
    values = jnp.stack([hess[:, :, n * part] for n in range(systems)])
    upper = jnp.transpose(values[:, :STEPS, :STEPS], (0, 2, 1))
    upper = jnp.concatenate([upper, jnp.zeros((systems, 1, STEPS), f32)], axis=1)
    below = values[:, 1:, 8]
    i = jnp.arange(STEPS + 1)[:, None]
    j = jnp.arange(STEPS)[None, :]
    hessenberg = jnp.where(i <= j, upper, jnp.where(i == j + 1, below[:, None, :], 0.0))
    return sol.reshape(systems, piece * width), hessenberg


def solution(mesh):
    return jax.shard_map(
        functools.partial(body, mesh.shape["row"], mesh.shape["col"]),
        mesh=mesh,
        in_specs=(
            P(("row", "col"), None, None),
            P(("row", "col"), None),
            P(("row", "col"), None),
            P(("row", "col")),
            P(None, ("row", "col")),
        ),
        out_specs=(P(None, ("row", "col")), P()),
        check_vma=False,
    )
```
